32 devices in a mesh: shard: 4 (over x, core), rep: 8 (over z, y).
Axes of the slice: x: 2, y: 2, z: 4, core: 2. Of those that a mesh axis runs over, the one named last changes fastest.
Arguments:
- tokens: bfloat16 [12288, 4608], P(('shard', 'rep')), may hold values from -6 to 6
- norm_gain: float32 [4608], replicated, may hold values from 0.25 to 1.75
- key_grad: bfloat16 [12288, 1024], P(('shard', 'rep')), may hold values from -6 to 6
- key_weight: bfloat16 [4608, 1024], P('shard'), may hold values from -0.09375 to 0.09375
- m_code: bfloat16 [4608, 1024], P('shard'), may hold values from -127 to 127, as said below
- m_exp: int32 [4608, 4], P('shard'), may hold values from 3 to 7
- v_code: bfloat16 [4608, 1024], P('shard'), may hold values from 1 to 255, as said below
- v_exp: int32 [4608, 4], P('shard'), may hold values from 4 to 9
Outputs:
- keys: bfloat16 [12288, 1024], P(('shard', 'rep'))
- token_grad: bfloat16 [12288, 4608], P(('shard', 'rep'))
- adam_step: float32 [4608, 1024], P('shard')
- m_rel: bfloat16 [4608, 1024], P('shard')
- m_scale: float32 [4608, 4], P('shard')
- v_rel: bfloat16 [4608, 1024], P('shard')
- v_scale: float32 [4608, 4], P('shard')
The draws below stay inside these ranges and needn't reach their ends.
Inputs may be any that keep to these rules, and one draw needn't show every extreme that they name: `m_code`: whole numbers. `v_code`: whole numbers.
All inputs are finite; a program needn't handle non-finite values. Where the reference program divides by a largest or mean magnitude, that divisor is 1e-20 or more.
Results may differ from the reference program's by a relative error of at most 0.0099.
Values may be sent and summed in bfloat16 or wider, within the bound.
A program may use at most 192 MiB of HBM per device.

```python
import jax
import jax.numpy as jnp
from jax import lax

D = 4608
KH = 1024
NB = 4
TOKENS = 12288


def draw_m_code(key, part):
    return jax.random.randint(key, (D, KH), -127, 128).astype(jnp.float32).astype(jnp.bfloat16)


def draw_v_code(key, part):
    return jax.random.randint(key, (D, KH), 1, 256).astype(jnp.float32).astype(jnp.bfloat16)


def place_ends(values, stream_key, smallest, largest):
    extent = values.shape
    index_at = [jax.random.randint(jax.random.fold_in(stream_key, axis), (), 0, extent[axis]) for axis in range(len(extent))]
    values = values.at[tuple(index_at)].set(smallest)
    longest = extent.index(max(extent))
    index_at[longest] = (index_at[longest] + 1) % extent[longest]
    return values.at[tuple(index_at)].set(largest)


def steps_of(own_key, dims, shards, smallest, largest):
    def one(dim, parts):
        steps = jax.random.uniform(jax.random.fold_in(jax.random.fold_in(own_key, 6), dim), (parts,), jnp.float32, smallest / len(shards), largest / len(shards))
        return jnp.repeat(jnp.exp(steps), dims[dim] // parts).reshape((-1,) + (1,) * (len(dims) - dim - 1))

    level = one(*shards[0])
    for cut in shards[1:]:
        level = level * one(*cut)
    return level


def bell_draw(stream_key, dims, scale, most, split=(), kind=jnp.bfloat16):
    drawn = scale * jax.random.normal(stream_key, dims, jnp.float32)
    if split:
        drawn = drawn * steps_of(stream_key, dims, split, -0.22, 0.18)
    return jnp.clip(drawn, -most, most).astype(kind)


def setup_inputs(seed: int = 0) -> dict:
    streams_of = jax.random.split(jax.random.key(seed), 9)
    return {
        "tokens": bell_draw(streams_of[0], (TOKENS, D), 1.0, 6.0, ((0, 32),)),
        "norm_gain": jnp.clip(1.0 + 0.15 * jax.random.normal(streams_of[1], (D,), jnp.float32), 0.25, 1.75),
        "key_grad": bell_draw(streams_of[2], (TOKENS, KH), 1.0, 6.0, ((0, 32),)),
        "key_weight": bell_draw(streams_of[3], (D, KH), D ** -0.5, 0.09375, ((0, 4),)),
        "m_code": draw_m_code(jax.random.fold_in(streams_of[8], 71), 0),
        "m_exp": place_ends(jax.random.randint(streams_of[5], (D, NB), 3, 8), jax.random.fold_in(streams_of[5], 1), 3, 7).astype(jnp.int32),
        "v_code": draw_v_code(jax.random.fold_in(streams_of[8], 71), 0),
        "v_exp": place_ends(jax.random.randint(streams_of[7], (D, NB), 4, 10), jax.random.fold_in(streams_of[7], 1), 4, 9).astype(jnp.int32),
    }


bias_first = 0.9999734386011124
bias_second = 0.0952078528862904

def requantize(grad, m_code, m_exp, v_code, v_exp):
    rows, width = grad.shape
    blocks = m_exp.shape[1]
    size = width // blocks
    g3 = grad.reshape(rows, blocks, size)
    m_old = m_code.astype(jnp.float32).reshape(rows, blocks, size) * (jnp.exp2(m_exp.astype(jnp.float32)) / 127.0)[:, :, None]
    v_old = v_code.astype(jnp.float32).reshape(rows, blocks, size) * (jnp.exp2(v_exp.astype(jnp.float32)) / 255.0)[:, :, None]
    m_new = 0.9 * m_old + 0.1 * g3
    v_new = 0.999 * v_old + 0.001 * g3 * g3
    step = m_new / bias_first / (jnp.sqrt(v_new / bias_second) + 1e-08)
    m_scale = lax.optimization_barrier(jnp.max(jnp.abs(m_new), axis=2))
    v_scale = lax.optimization_barrier(jnp.max(v_new, axis=2))
    m_rel = (m_new / (m_scale + 1e-06)[:, :, None]).reshape(rows, width).astype(jnp.bfloat16)
    v_rel = (v_new / (v_scale + 1e-06)[:, :, None]).reshape(rows, width).astype(jnp.bfloat16)
    return (step.reshape(rows, width), m_rel, m_scale, v_rel, v_scale)

def reference(tokens, norm_gain, key_grad, key_weight, m_code, m_exp, v_code, v_exp):
    x = tokens.astype(jnp.float32)
    inv = lax.rsqrt(lax.optimization_barrier(jnp.mean(x * x, axis=1, keepdims=True)) + 1e-06)
    normed = (x * inv * norm_gain).astype(jnp.bfloat16)
    keys = jnp.dot(normed, key_weight, preferred_element_type=jnp.float32).astype(jnp.bfloat16)
    dnormed = lax.dot_general(key_grad, key_weight, (((1,), (1,)), ((), ())), preferred_element_type=jnp.float32)
    scaled = dnormed * norm_gain
    inner = lax.optimization_barrier(jnp.mean(scaled * x, axis=1, keepdims=True))
    token_grad = (inv * scaled - x * inv * inv * inv * inner).astype(jnp.bfloat16)
    grad = lax.dot_general(normed, key_grad, (((0,), (0,)), ((), ())), preferred_element_type=jnp.float32)
    step, m_rel, m_scale, v_rel, v_scale = requantize(grad, m_code, m_exp, v_code, v_exp)
    return (keys, token_grad, step, m_rel, m_scale, v_rel, v_scale)
```

```python
import functools

import jax
import jax.numpy as jnp
from jax import lax
from jax.sharding import PartitionSpec as P

bias_first = 0.9999734386011124
bias_second = 0.0952078528862904


def requantize(grad, m_code, m_exp, v_code, v_exp):
    rows, width = grad.shape
    blocks = m_exp.shape[1]
    size = width // blocks
    g3 = grad.reshape(rows, blocks, size)
    m_old = (
        m_code.astype(jnp.float32).reshape(rows, blocks, size)
        * (jnp.exp2(m_exp.astype(jnp.float32)) / 127.0)[:, :, None]
    )
    v_old = (
        v_code.astype(jnp.float32).reshape(rows, blocks, size)
        * (jnp.exp2(v_exp.astype(jnp.float32)) / 255.0)[:, :, None]
    )
    m_new = 0.9 * m_old + 0.1 * g3
    v_new = 0.999 * v_old + 0.001 * g3 * g3
    step = m_new / bias_first / (jnp.sqrt(v_new / bias_second) + 1e-08)
    m_scale = jnp.max(jnp.abs(m_new), axis=2)
    v_scale = jnp.max(v_new, axis=2)
    m_rel = (m_new / (m_scale + 1e-06)[:, :, None]).reshape(rows, width).astype(jnp.bfloat16)
    v_rel = (v_new / (v_scale + 1e-06)[:, :, None]).reshape(rows, width).astype(jnp.bfloat16)
    return (step.reshape(rows, width), m_rel, m_scale, v_rel, v_scale)


def bit_of(axis, bit):
    return lax.rem(lax.div(lax.axis_index(axis), 2**bit), 2)


def swap(value, axis, bit, count):
    return lax.ppermute(value, axis, [(i, i ^ (1 << bit)) for i in range(count)])


def bits_of(count):
    bits = count.bit_length() - 1
    assert 1 << bits == count
    return bits


def pick(value, index, dim):
    return lax.dynamic_index_in_dim(value, index, dim, keepdims=False)


def halve(value, labels, label, counts):
    axis, bit = label
    dim = labels.index(label)
    mine = bit_of(axis, bit)
    came = swap(pick(value, 1 - mine, dim), axis, bit, counts[axis])
    kept = pick(value, mine, dim)
    total = (kept.astype(jnp.float32) + came.astype(jnp.float32)).astype(jnp.bfloat16)
    return total, [other for other in labels if other != label]


def double(value, labels, label, counts):
    axis, bit = label
    mine = bit_of(axis, bit)
    came = swap(value, axis, bit, counts[axis])
    dim = sum(1 for other in labels if other[1] > bit)
    low = jnp.where(mine == 0, value, came)
    high = jnp.where(mine == 0, came, value)
    return jnp.stack([low, high], axis=dim), labels[:dim] + [label] + labels[dim:]


def gather_weight(weight, counts):
    shards = bits_of(counts["shard"])
    reps = bits_of(counts["rep"])
    rows, width = weight.shape
    near = swap(weight, "shard", 0, counts["shard"])
    core = bit_of("shard", 0)
    pair = jnp.stack([jnp.where(core == 0, weight, near), jnp.where(core == 0, near, weight)])
    helpers = list(range(min(reps, 2)))
    labels, value = [("shard", 0)], pair
    own = weight
    for bit in range(1, shards):
        pieces = []
        parts = own.reshape((len(helpers),) + (2, rows // (2 * len(helpers))) + (width,)) if bit == 1 else None
        if bit == 1:
            for n, helper in enumerate(helpers):
                part = parts[n]
                side = bit_of("rep", helper)
                half = swap(pick(part, side, 0), "shard", bit, counts["shard"])
                rest = swap(half, "rep", helper, counts["rep"])
                pieces.append(jnp.where(side == 0, half, rest))
                pieces.append(jnp.where(side == 0, rest, half))
            far = jnp.concatenate(pieces, axis=0)
            other = swap(far, "shard", 0, counts["shard"])
            came = jnp.stack([jnp.where(core == 0, far, other), jnp.where(core == 0, other, far)])
        else:
            came = swap(value, "shard", bit, counts["shard"])
        mine = bit_of("shard", bit)
        value = jnp.stack([jnp.where(mine == 0, value, came), jnp.where(mine == 0, came, value)])
    return value.reshape(counts["shard"] * rows, width)


def body(counts, tokens, norm_gain, key_grad, key_weight, m_code, m_exp, v_code, v_exp):
    shards = bits_of(counts["shard"])
    reps = bits_of(counts["rep"])
    features = tokens.shape[1]
    width = key_grad.shape[1]
    chunks = m_exp.shape[1]
    size = width // chunks
    x = tokens.astype(jnp.float32)
    inv = lax.rsqrt(jnp.mean(x * x, axis=1, keepdims=True) + 1e-06)
    normed = (x * inv * norm_gain).astype(jnp.bfloat16)

    rows = features // counts["shard"]
    split = normed.reshape(normed.shape[0], counts["shard"] // 2, 2, rows)
    core = bit_of("shard", 0)
    theirs = pick(split, 1 - core, 2).reshape(normed.shape[0], -1)
    ours = pick(split, core, 2).reshape(normed.shape[0], -1)
    far = [("shard", bit) for bit in range(shards - 1, 0, -1)]
    reverse = [("rep", bit) for bit in range(reps - 1, -1, -1)]
    near = reverse[::-1]
    orders = [far + near, near[:1] + far + near[1:], near[1:2] + far + near[:1] + near[2:], near[1:2] + near[:1] + far + near[2:]]

    def outer(columns, c):
        part = lax.slice_in_dim(key_grad, c * size, (c + 1) * size, axis=1)
        return lax.dot_general(columns, part, (((0,), (0,)), ((), ())), preferred_element_type=jnp.float32)

    sent = [swap(outer(theirs, c).astype(jnp.bfloat16), "shard", 0, counts["shard"]) for c in range(chunks)]
    weight = gather_weight(key_weight, counts)
    totals = []
    for c in range(chunks):
        total = (outer(ours, c) + sent[c].astype(jnp.float32)).astype(jnp.bfloat16)
        labels = far + reverse
        total = total.reshape([2] * len(labels) + [rows // counts["rep"], size])
        for label in orders[c % len(orders)]:
            total, labels = halve(total, labels, label, counts)
        for label in reverse:
            total, labels = double(total, labels, label, counts)
        totals.append(total.reshape(rows, size))
    grad = jnp.concatenate(totals, axis=1).astype(jnp.float32)

    keys = jnp.dot(normed, weight, preferred_element_type=jnp.float32).astype(jnp.bfloat16)
    back = lax.dot_general(
        key_grad, weight, (((1,), (1,)), ((), ())), preferred_element_type=jnp.float32
    )
    scaled = back * norm_gain
    inner = jnp.mean(scaled * x, axis=1, keepdims=True)
    token_grad = (inv * scaled - x * inv * inv * inv * inner).astype(jnp.bfloat16)
    step, m_rel, m_scale, v_rel, v_scale = requantize(grad, m_code, m_exp, v_code, v_exp)
    return (keys, token_grad, step, m_rel, m_scale, v_rel, v_scale)


def solution(mesh):
    return jax.shard_map(
        functools.partial(body, dict(mesh.shape)),
        mesh=mesh,
        in_specs=(
            P(("shard", "rep"), None),
            P(),
            P(("shard", "rep"), None),
            P("shard", None),
            P("shard", None),
            P("shard", None),
            P("shard", None),
            P("shard", None),
        ),
        out_specs=(
            P(("shard", "rep"), None),
            P(("shard", "rep"), None),
            P("shard", None),
            P("shard", None),
            P("shard", None),
            P("shard", None),
            P("shard", None),
        ),
        check_vma=False,
    )
```

```python
import functools

import jax
import jax.numpy as jnp
from jax import lax
from jax.experimental import pallas as pl
from jax.experimental.pallas import tpu as pltpu
from jax.sharding import PartitionSpec as P


bias_first = 0.9999734386011124
bias_second = 0.0952078528862904


def requantize_kernel(chunks, rep_ref, *refs):
    grads = refs[:chunks]
    m_code, m_unit, v_code, v_unit, step, m_rel, m_scale, v_rel, v_scale = refs[chunks:]
    size = m_code.shape[1] // chunks
    for c in range(chunks):
        cols = slice(c * size, (c + 1) * size)
        one = slice(c, c + 1)
        g = grads[c][...].astype(jnp.float32)
        m_old = m_code[:, cols].astype(jnp.float32) * m_unit[:, one]
        v_old = v_code[:, cols].astype(jnp.float32) * v_unit[:, one]
        m_new = 0.9 * m_old + 0.1 * g
        v_new = 0.999 * v_old + 0.001 * g * g
        step[:, cols] = m_new / bias_first / (jnp.sqrt(v_new / bias_second) + 1e-08)
        m_top = jnp.max(jnp.abs(m_new), axis=1, keepdims=True)
        v_top = jnp.max(v_new, axis=1, keepdims=True)
        m_scale[:, one] = m_top
        v_scale[:, one] = v_top
        m_rel[:, cols] = (m_new / (m_top + 1e-06)).astype(jnp.bfloat16)
        v_rel[:, cols] = (v_new / (v_top + 1e-06)).astype(jnp.bfloat16)


def requantize(grads, bits, m_code, m_exp, v_code, v_exp):
    count, part, size = grads[0].shape
    chunks = len(grads)
    rows, width = m_code.shape
    m_unit = jnp.exp2(m_exp.astype(jnp.float32)) / 127.0
    v_unit = jnp.exp2(v_exp.astype(jnp.float32)) / 255.0
    cut = lambda a: a.reshape(count, part, a.shape[1])

    def came_at(i, rep_ref):
        apart = i ^ rep_ref[0]
        place = jnp.int32(0)
        for k, bit in enumerate(bits):
            place = place + (((apart >> bit) & 1) << k)
        return (place, 0, 0)

    grad_spec = pl.BlockSpec((None, part, size), came_at)
    wide = pl.BlockSpec((None, part, width), lambda i, rep_ref: (i, 0, 0))
    thin = pl.BlockSpec((None, part, chunks), lambda i, rep_ref: (i, 0, 0))
    shape = lambda w, kind: jax.ShapeDtypeStruct((count, part, w), kind)
    outs = pl.pallas_call(
        functools.partial(requantize_kernel, chunks),
        grid_spec=pltpu.PrefetchScalarGridSpec(
            num_scalar_prefetch=1,
            grid=(count,),
            in_specs=[grad_spec] * chunks + [wide, thin, wide, thin],
            out_specs=[wide, wide, thin, wide, thin],
        ),
        out_shape=[
            shape(width, jnp.float32),
            shape(width, jnp.bfloat16),
            shape(chunks, jnp.float32),
            shape(width, jnp.bfloat16),
            shape(chunks, jnp.float32),
        ],
        cost_estimate=pl.CostEstimate(flops=20 * rows * width, bytes_accessed=14 * rows * width, transcendentals=rows * width),
    )(lax.axis_index("rep").astype(jnp.int32).reshape(1), *grads, cut(m_code), cut(m_unit), cut(v_code), cut(v_unit))
    return tuple(out.reshape(rows, out.shape[2]) for out in outs)


def bit_of(axis, bit):
    return lax.rem(lax.div(lax.axis_index(axis), 2**bit), 2)


def swap(value, axis, bit, count):
    return lax.ppermute(value, axis, [(i, i ^ (1 << bit)) for i in range(count)])


def bits_of(count):
    bits = count.bit_length() - 1
    assert 1 << bits == count
    return bits


def pick(value, index, dim):
    return lax.dynamic_index_in_dim(value, index, dim, keepdims=False)


def halve(value, labels, label, counts):
    axis, bit = label
    dim = labels.index(label)
    mine = bit_of(axis, bit)
    came = swap(pick(value, 1 - mine, dim).astype(jnp.bfloat16), axis, bit, counts[axis])
    total = pick(value, mine, dim) + came.astype(jnp.float32)
    return total, [other for other in labels if other != label]


def double(value, label, counts):
    axis, bit = label
    return jnp.concatenate([value, swap(value, axis, bit, counts[axis])], axis=0)


def gather_weight(weight, counts):
    shards = bits_of(counts["shard"])
    reps = bits_of(counts["rep"])
    rows, width = weight.shape
    near = swap(weight, "shard", 0, counts["shard"])
    core = bit_of("shard", 0)
    pair = jnp.stack([jnp.where(core == 0, weight, near), jnp.where(core == 0, near, weight)])
    helpers = list(range(min(reps, 2)))
    value = pair
    own = weight
    for bit in range(1, shards):
        pieces = []
        parts = own.reshape((len(helpers),) + (2, rows // (2 * len(helpers))) + (width,)) if bit == 1 else None
        if bit == 1:
            for n, helper in enumerate(helpers):
                part = parts[n]
                side = bit_of("rep", helper)
                half = swap(pick(part, side, 0), "shard", bit, counts["shard"])
                rest = swap(half, "rep", helper, counts["rep"])
                pieces.append(jnp.where(side == 0, half, rest))
                pieces.append(jnp.where(side == 0, rest, half))
            far = jnp.concatenate(pieces, axis=0)
            other = swap(far, "shard", 0, counts["shard"])
            came = jnp.stack([jnp.where(core == 0, far, other), jnp.where(core == 0, other, far)])
        else:
            came = swap(value, "shard", bit, counts["shard"])
        mine = bit_of("shard", bit)
        value = jnp.stack([jnp.where(mine == 0, value, came), jnp.where(mine == 0, came, value)])
    return value.reshape(counts["shard"] * rows, width)


def whole(counts, tokens, norm_gain, key_grad, key_weight, m_code, m_exp, v_code, v_exp):
    shards = bits_of(counts["shard"])
    reps = bits_of(counts["rep"])
    features = tokens.shape[1]
    width = key_grad.shape[1]
    chunks = m_exp.shape[1]
    size = width // chunks
    x = tokens.astype(jnp.float32)
    inv = lax.rsqrt(jnp.mean(x * x, axis=1, keepdims=True) + 1e-06)
    normed = (x * inv * norm_gain).astype(jnp.bfloat16)

    later, inv = lax.optimization_barrier((tokens, inv))

    rows = features // counts["shard"]
    split = normed.reshape(normed.shape[0], counts["shard"] // 2, 2, rows)
    core = bit_of("shard", 0)
    theirs = pick(split, 1 - core, 2).reshape(normed.shape[0], -1)
    ours = pick(split, core, 2).reshape(normed.shape[0], -1)
    far = [("shard", bit) for bit in range(shards - 1, 0, -1)]
    reverse = [("rep", bit) for bit in range(reps - 1, -1, -1)]
    near = reverse[::-1]
    orders = [far + near, near[:1] + far + near[1:], near[1:2] + far + near[:1] + near[2:], near[1:2] + near[:1] + far + near[2:]]

    def outer(columns, c):
        part = lax.slice_in_dim(key_grad, c * size, (c + 1) * size, axis=1)
        return lax.dot_general(columns, part, (((0,), (0,)), ((), ())), preferred_element_type=jnp.float32)

    sent = []
    for c in range(chunks):
        part = outer(theirs, c).astype(jnp.bfloat16)
        sent.append(swap(part, "shard", 0, counts["shard"]))
    weight = gather_weight(key_weight, counts)
    totals = []
    for c in range(chunks):
        total = outer(ours, c) + sent[c].astype(jnp.float32)
        labels = far + reverse
        total = total.reshape([2] * len(labels) + [rows // counts["rep"], size])
        for label in orders[c % len(orders)]:
            total, labels = halve(total, labels, label, counts)
        total = total.astype(jnp.bfloat16)[None]
        for label in reverse:
            total = double(total, label, counts)
        totals.append(total)

    keys = jnp.dot(normed, weight, preferred_element_type=jnp.float32).astype(jnp.bfloat16)
    back = lax.dot_general(
        key_grad, weight, (((1,), (1,)), ((), ())), preferred_element_type=jnp.float32
    )
    scaled = back * norm_gain
    x = later.astype(jnp.float32)
    inner = jnp.mean(scaled * x, axis=1, keepdims=True)
    token_grad = (inv * scaled - x * inv * inv * inv * inner).astype(jnp.bfloat16)
    step, m_rel, m_scale, v_rel, v_scale = requantize(totals, [label[1] for label in reverse], m_code, m_exp, v_code, v_exp)
    return (keys, token_grad, step, m_rel, m_scale, v_rel, v_scale)


def body(counts, *arrays):
    return whole(counts, *arrays)


def solution(mesh):
    return jax.shard_map(
        functools.partial(body, dict(mesh.shape)),
        mesh=mesh,
        in_specs=(
            P(("shard", "rep"), None),
            P(),
            P(("shard", "rep"), None),
            P("shard", None),
            P("shard", None),
            P("shard", None),
            P("shard", None),
            P("shard", None),
        ),
        out_specs=(
            P(("shard", "rep"), None),
            P(("shard", "rep"), None),
            P("shard", None),
            P("shard", None),
            P("shard", None),
            P("shard", None),
            P("shard", None),
        ),
        check_vma=False,
    )
```
